32 devices in a mesh: tok: 4 (over x, core), exp: 8 (over z, y).
Axes of the slice: x: 2, y: 2, z: 4, core: 2. Of those that a mesh axis runs over, the one named last changes fastest.
Arguments:
- tokens: bfloat16 [8, 1024, 1024], P('exp', 'tok'), may hold values from -6 to 6
- upstream: bfloat16 [8, 1024, 1024], P('exp', 'tok'), may hold values from -6 to 6
- dispatch: bfloat16 [8, 1024, 8], P('exp', 'tok'), may hold values from 0 to 1, as said below
- combine: bfloat16 [8, 1024, 8], P('exp', 'tok'), may hold values from 0 to 1, as said below
- w_in: bfloat16 [8, 1024, 2048], P('exp', None, 'tok'), may hold values from -0.1875 to 0.1875
- w_out: bfloat16 [8, 2048, 1024], P('exp', 'tok'), may hold values from -0.125 to 0.125
- slot_keys: bfloat16 [1024, 8], replicated, may hold values from -0.1875 to 0.1875
Outputs:
- token_grad: bfloat16 [8, 1024, 1024], P('exp', 'tok')
The draws below stay inside these ranges and needn't reach their ends.
Inputs may be any that keep to these rules, and one draw needn't show every extreme that they name: `dispatch`: for each image and slot the entries over the image's tokens are positive and sum to one up to rounding. `combine`: for each token the entries over the 8 slots are positive and sum to one up to rounding.
All inputs are finite; a program needn't handle non-finite values.
Results may differ from the reference program's by a relative error of at most 0.025.
Values may be sent and summed in bfloat16 or wider, within the bound.
A program may use at most 64 MiB of HBM per device.

```python
import jax
import jax.numpy as jnp
from jax import lax

D = 1024
HID = 2048
PATCHES = 1024
EXPERTS = 8
IMAGES = 8
N_TOK = 4
N_EXP = 8


def draw_dispatch(key, part):
    logits = jax.random.normal(jax.random.fold_in(key, 11), (IMAGES, PATCHES, EXPERTS), jnp.float32)
    logits = 2.5 * logits
    return jax.nn.softmax(logits, axis=1).astype(jnp.bfloat16)


def draw_combine(key, part):
    logits = jax.random.normal(jax.random.fold_in(key, 21), (IMAGES, PATCHES, EXPERTS), jnp.float32)
    logits = 1.5 * logits
    return jax.nn.softmax(logits, axis=2).astype(jnp.bfloat16)


def steps_of(stream_key, dims, split, low, largest):
    def one(axis_at, blocks):
        heights = jax.random.uniform(jax.random.fold_in(jax.random.fold_in(stream_key, 6), axis_at), (blocks,), jnp.float32, low / len(split), largest / len(split))
        return jnp.repeat(jnp.exp(heights), dims[axis_at] // blocks).reshape((-1,) + (1,) * (len(dims) - axis_at - 1))

    level = one(*split[0])
    for cut in split[1:]:
        level = level * one(*cut)
    return level


def scatter_about(key, extent, spread, most, pieces=(), dtype=jnp.bfloat16):
    values = spread * jax.random.normal(key, extent, jnp.float32)
    if pieces:
        values = values * steps_of(key, extent, pieces, -0.22, 0.18)
    return jnp.clip(values, -most, most).astype(dtype)


def setup_inputs(seed: int = 0) -> dict:
    keys = jax.random.split(jax.random.key(seed), 8)
    tokens = scatter_about(keys[0], (IMAGES, PATCHES, D), 1.0, 6.0, ((0, 8), (1, 4)))
    upstream = scatter_about(keys[1], (IMAGES, PATCHES, D), 1.0, 6.0, ((0, 8), (1, 4)))
    dispatch = draw_dispatch(jax.random.fold_in(keys[7], 71), 0)
    combine = draw_combine(jax.random.fold_in(keys[7], 71), 0)
    w_in = scatter_about(keys[4], (EXPERTS, D, HID), D ** -0.5, 0.1875, ((0, 8), (2, 4)))
    w_out = scatter_about(keys[5], (EXPERTS, HID, D), HID ** -0.5, 0.125, ((0, 8), (1, 4)))
    slot_keys = scatter_about(keys[6], (D, EXPERTS), D ** -0.5, 0.1875)
    return dict(tokens=tokens, upstream=upstream, dispatch=dispatch, combine=combine, w_in=w_in, w_out=w_out, slot_keys=slot_keys)


def gelu_parts(pre_act):
    inside = 0.7978845608 * (pre_act + 0.044715 * pre_act * pre_act * pre_act)
    tanh_val = jnp.tanh(inside)
    gelu_value = 0.5 * pre_act * (1.0 + tanh_val)
    gelu_slope = 0.5 * (1.0 + tanh_val) + 0.5 * pre_act * (1.0 - tanh_val * tanh_val) * 0.7978845608 * (1.0 + 3.0 * 0.044715 * pre_act * pre_act)
    return gelu_value, gelu_slope


def group_total(partials):
    rounded = lax.optimization_barrier(partials.astype(jnp.bfloat16))
    return jnp.sum(rounded.astype(jnp.float32), axis=0).astype(jnp.bfloat16)


def reference(tokens, upstream, dispatch, combine, w_in, w_out, slot_keys):
    shard = PATCHES // N_TOK
    hidden_split = HID // N_TOK

    def token_forward(items):
        tok_image, grad_image, disp_image, comb_image = items
        tok_groups = tok_image.astype(jnp.float32).reshape(N_TOK, shard, D)
        grad_groups = grad_image.astype(jnp.float32).reshape(N_TOK, shard, D)
        disp_groups = disp_image.astype(jnp.float32).reshape(N_TOK, shard, N_EXP)
        comb_groups = comb_image.astype(jnp.float32).reshape(N_TOK, shard, N_EXP)
        slot_input = group_total(jnp.einsum("tms,tmd->tsd", disp_groups, tok_groups))
        slot_grad = group_total(jnp.einsum("tms,tmd->tsd", comb_groups, grad_groups))
        return slot_input, slot_grad

    slot_input, slot_grad = lax.map(token_forward, (tokens, upstream, dispatch, combine))

    def expert_step(items):
        input_rows, grad_rows, w_first, w_second = items
        first_groups = w_first.astype(jnp.float32).reshape(D, N_TOK, hidden_split)
        second_groups = w_second.astype(jnp.float32).reshape(N_TOK, hidden_split, D)
        pre_act = jnp.einsum("bd,dth->tbh", input_rows.astype(jnp.float32), first_groups)
        gelu_value, gelu_slope = gelu_parts(pre_act)
        hidden = gelu_value.astype(jnp.bfloat16).astype(jnp.float32)
        slot_output = group_total(jnp.einsum("tbh,thd->tbd", hidden, second_groups))
        hidden_grad = jnp.einsum("bd,thd->tbh", grad_rows.astype(jnp.float32), second_groups)
        pre_grad = (hidden_grad * gelu_slope).astype(jnp.bfloat16).astype(jnp.float32)
        slot_back = group_total(jnp.einsum("tbh,dth->tbd", pre_grad, first_groups))
        return slot_output, slot_back

    slot_output, slot_back = lax.map(expert_step, (jnp.transpose(slot_input, (1, 0, 2)), jnp.transpose(slot_grad, (1, 0, 2)), w_in, w_out))
    slot_output = jnp.transpose(slot_output, (1, 0, 2))
    slot_back = jnp.transpose(slot_back, (1, 0, 2))

    def token_backward(items):
        tok_image, grad_image, disp_image, comb_image, output_image, back_image = items
        comb_grad = jnp.dot(grad_image, output_image.T, preferred_element_type=jnp.float32)
        disp_grad = jnp.dot(tok_image, back_image.T, preferred_element_type=jnp.float32)
        comb_full = comb_image.astype(jnp.float32)
        disp_full = disp_image.astype(jnp.float32)
        comb_logit = comb_full * (comb_grad - jnp.sum(comb_full * comb_grad, axis=1, keepdims=True))
        totals = jnp.sum(disp_full * disp_grad, axis=0, keepdims=True)
        disp_logit = disp_full * (disp_grad - totals)
        logit_grad = (comb_logit + disp_logit).astype(jnp.bfloat16)
        result = jnp.dot(disp_image, back_image, preferred_element_type=jnp.float32)
        result = result + jnp.dot(logit_grad, slot_keys.T, preferred_element_type=jnp.float32)
        return result.astype(jnp.bfloat16)

    return lax.map(token_backward, (tokens, upstream, dispatch, combine, slot_output, slot_back))
```

```python
import functools

import jax
import jax.numpy as jnp
from jax import lax
from jax.experimental import pallas as pl
from jax.experimental.pallas import tpu as pltpu
from jax.sharding import PartitionSpec as P

MESH = pl.DeviceIdType.MESH
LANES = 128
NT = (((1,), (1,)), ((), ()))
NN = (((1,), (0,)), ((), ()))
TN = (((0,), (0,)), ((), ()))


def gelu_parts(pre_act):
    inside = 0.7978845608 * (pre_act + 0.044715 * pre_act * pre_act * pre_act)
    tanh_val = jnp.tanh(inside)
    gelu_value = 0.5 * pre_act * (1.0 + tanh_val)
    gelu_slope = 0.5 * (1.0 + tanh_val) + 0.5 * pre_act * (
        1.0 - tanh_val * tanh_val
    ) * 0.7978845608 * (1.0 + 3.0 * 0.044715 * pre_act * pre_act)
    return (gelu_value, gelu_slope)


def mm(a, b, dims):
    return lax.dot_general(a, b, dims, preferred_element_type=jnp.float32)


def partner(me, k, count):
    if count & (count - 1):
        return lax.rem(me + k, count)
    for bit in range(count.bit_length() - 1):
        if k >> bit & 1:
            me = me + (1 << bit) * (1 - 2 * (me // (1 << bit) % 2))
    return me


def kernel(
    n_tok, n_exp,
    tok_hbm, up_hbm, disp_hbm, comb_hbm, win_hbm, wout_hbm, keys_hbm,
    left_ref, right_ref,
    tok, up, disp, comb, win, wout, keys, tok_t, up_t, win_t, wout_t,
    rows, send1, recv1, send2, recv2, part, parts,
    load_sem, send_sem, recv_sem,
):
    t_me, e_me = lax.axis_index("tok"), lax.axis_index("exp")
    me = t_me * n_exp + e_me
    n_dev = n_tok * n_exp
    width = tok.shape[1]
    chunks = width // LANES

    loads = [
        pltpu.make_async_copy(src, dst, load_sem.at[k])
        for k, (src, dst) in enumerate((
            (disp_hbm, disp), (tok_hbm, tok), (comb_hbm, comb), (up_hbm, up),
            (win_hbm, win), (wout_hbm, wout), (keys_hbm, keys),
        ))
    ]

    barrier = pltpu.get_barrier_semaphore()

    def others(act):
        if n_exp <= 16:
            for dt in reversed(range(n_tok)):
                for k in reversed(range(n_exp)):
                    if k or dt:
                        act(partner(t_me, dt, n_tok), partner(e_me, k, n_exp))
            return

        @pl.loop(0, n_exp)
        def _(k):
            e = lax.rem(e_me + k, n_exp)
            for dt in range(1, n_tok):
                act(lax.rem(t_me + dt, n_tok), e)
            pl.when(k > 0)(functools.partial(act, t_me, e))

    others(lambda t, e: pl.semaphore_signal(
        barrier, inc=1, device_id=(t, e), device_id_type=MESH))
    for copy in loads:
        copy.start()

    def spread(first, second):
        for j in range(chunks):
            cut = slice(j * LANES, (j + 1) * LANES)
            rows[pl.ds(j, n_exp, stride=2 * chunks), :] = first[:, cut]
            rows[pl.ds(chunks + j, n_exp, stride=2 * chunks), :] = second[:, cut]
        return rows[...].reshape(n_exp, 2 * chunks, LANES).astype(jnp.bfloat16)

    def gather(which):
        return jnp.concatenate(
            [rows[pl.ds(which * chunks + j, n_exp, stride=2 * chunks), :] for j in range(chunks)],
            axis=1,
        )

    def towards(act):
        dests = [(t, e) for t in range(n_tok) for e in range(n_exp)]
        for t, e in sorted(dests, key=lambda d: bin(d[0] >> 1).count("1") + d[1] // 2 + d[1] % 2):
            pl.when((t_me != t) | (e_me != e))(functools.partial(act, t, e))

    def exchange(send, recv, way):
        def act(t, e):
            pltpu.make_async_remote_copy(
                src_ref=send.at[e], dst_ref=recv.at[me],
                send_sem=send_sem.at[way], recv_sem=recv_sem.at[way],
                device_id=(t, e), device_id_type=MESH,
            ).start()
        if way and n_exp <= 16:
            towards(act)
        else:
            others(act)

    def arrived(recv, way):
        some = recv.at[pl.ds(0, n_dev - 1)]
        pltpu.make_async_copy(some, some, recv_sem.at[way]).wait()
        total = jnp.zeros((n_exp, 2 * chunks, LANES), jnp.float32)
        for t in range(n_tok):
            total = total + recv[pl.ds(t * n_exp, n_exp)].astype(jnp.float32)
        rows[...] = total.reshape(n_exp * 2 * chunks, LANES)
        return gather(0).astype(jnp.bfloat16), gather(1).astype(jnp.bfloat16)

    loads[0].wait()
    loads[1].wait()
    slot_in = mm(disp[...], tok[...], NN)
    loads[2].wait()
    loads[3].wait()
    slot_grad = mm(comb[...], up[...], NN)
    slabs = spread(slot_in, slot_grad)
    send1[...] = slabs
    recv1[me] = send1[e_me]
    part[...] = slot_in.astype(jnp.bfloat16)
    parts[t_me] = part[...]
    pl.semaphore_wait(barrier, n_dev - 1)
    exchange(send1, recv1, 0)
    for dt in range(1, n_tok):
        pltpu.make_async_remote_copy(
            src_ref=part, dst_ref=parts.at[t_me],
            send_sem=send_sem.at[2], recv_sem=recv_sem.at[2],
            device_id=(lax.rem(t_me + dt, n_tok), e_me), device_id_type=MESH,
        ).start()
    loads[4].wait()
    loads[5].wait()
    loads[6].wait()
    wout_t[...] = wout[...].T
    win_t[...] = win[...].T

    in_rows, grad_rows = arrived(recv1, 0)
    pre_act = mm(in_rows, win[...], NN)
    hidden_grad = mm(grad_rows, wout_t[...], NN)
    gelu_value, gelu_slope = gelu_parts(pre_act)
    slot_out = mm(gelu_value.astype(jnp.bfloat16), wout[...], NN)
    slot_back = mm((hidden_grad * gelu_slope).astype(jnp.bfloat16), win_t[...], NN)
    send2[...] = spread(slot_out, slot_back)
    recv2[me] = send2[e_me]
    exchange(send2, recv2, 1)

    some = parts.at[pl.ds(0, n_tok - 1)]
    pltpu.make_async_copy(some, some, recv_sem.at[2]).wait()
    tok_t[...] = tok[...].T
    up_t[...] = up[...].T
    in_total = parts[0].astype(jnp.float32)
    for t in range(1, n_tok):
        in_total = in_total + parts[t].astype(jnp.float32)

    out_rows, back_rows = arrived(recv2, 1)
    comb_grad = mm(out_rows, up_t[...], NN)
    disp_grad = mm(back_rows, tok_t[...], NN)
    totals = jnp.sum(in_total * back_rows.astype(jnp.float32), axis=1, keepdims=True)
    comb_full = comb[...].astype(jnp.float32)
    disp_full = disp[...].astype(jnp.float32)
    comb_logit = comb_full * (comb_grad - jnp.sum(comb_full * comb_grad, axis=0, keepdims=True))
    logit_grad = comb_logit + disp_full * (disp_grad - totals)
    left = jnp.concatenate([disp_full, logit_grad], axis=0).astype(jnp.bfloat16)
    right = jnp.concatenate(
        [back_rows.astype(jnp.float32), keys[...].astype(jnp.float32)], axis=0
    ).astype(jnp.bfloat16)
    left_ref[...] = left
    right_ref[...] = right

    for way, sent in enumerate((recv1.at[pl.ds(0, n_dev - 1)], recv2.at[pl.ds(0, n_dev - 1)], some)):
        pltpu.make_async_copy(sent, sent, send_sem.at[way]).wait()


def finish(left, right, out_hbm, held, sem):
    pieces = 4
    count = held.shape[0] // pieces
    copies = []
    for k in range(pieces):
        cut = slice(k * count, (k + 1) * count)
        held[cut] = mm(left[:, cut], right[...], TN).astype(jnp.bfloat16)
        copies.append(pltpu.make_async_copy(held.at[cut], out_hbm.at[cut], sem.at[k]))
        copies[-1].start()
    for copy in copies:
        copy.wait()


def solution(mesh):
    n_tok, n_exp = mesh.shape["tok"], mesh.shape["exp"]

    def body(tokens, upstream, dispatch, combine, w_in, w_out, slot_keys):
        args = (
            tokens[0], upstream[0], dispatch[0].T, combine[0].T, w_in[0], w_out[0], slot_keys.T,
        )
        count, width = args[0].shape
        slab = (2 * width // LANES, LANES)
        bf16 = jnp.bfloat16
        left, right = pl.pallas_call(
            functools.partial(kernel, n_tok, n_exp),
            out_shape=(jax.ShapeDtypeStruct((2 * n_exp, count), bf16), jax.ShapeDtypeStruct((2 * n_exp, width), bf16)),
            in_specs=[pl.BlockSpec(memory_space=pltpu.HBM)] * len(args),
            out_specs=(pl.BlockSpec(memory_space=pltpu.VMEM),) * 2,
            scratch_shapes=[pltpu.VMEM(a.shape, bf16) for a in args] + [
                pltpu.VMEM(args[k].shape[::-1], bf16) for k in (0, 1, 4, 5)
            ] + [
                pltpu.VMEM((n_exp * slab[0], LANES), jnp.float32),
                pltpu.VMEM((n_exp,) + slab, bf16),
                pltpu.VMEM((n_tok * n_exp,) + slab, bf16),
                pltpu.VMEM((n_exp,) + slab, bf16),
                pltpu.VMEM((n_tok * n_exp,) + slab, bf16),
                pltpu.VMEM((n_exp, width), bf16),
                pltpu.VMEM((n_tok, n_exp, width), bf16),
                pltpu.SemaphoreType.DMA((len(args),)),
                pltpu.SemaphoreType.DMA((3,)),
                pltpu.SemaphoreType.DMA((3,)),
            ],
            compiler_params=pltpu.CompilerParams(
                collective_id=0, has_side_effects=True, vmem_limit_bytes=40 << 20
            ),
            name="soft_moe_back",
        )(*[pltpu.with_memory_space_constraint(a, pltpu.HBM) for a in args])
        result = pl.pallas_call(
            finish,
            out_shape=jax.ShapeDtypeStruct((count, width), bf16),
            in_specs=[pl.BlockSpec(memory_space=pltpu.VMEM)] * 2,
            out_specs=pl.BlockSpec(memory_space=pltpu.HBM),
            scratch_shapes=[pltpu.VMEM((count, width), bf16), pltpu.SemaphoreType.DMA((4,))],
            compiler_params=pltpu.CompilerParams(vmem_limit_bytes=4 << 20),
            name="finish",
        )(left, right)
        return result[None]

    placed = (
        P("exp", "tok", None),
        P("exp", "tok", None),
        P("exp", "tok", None),
        P("exp", "tok", None),
        P("exp", None, "tok"),
        P("exp", "tok", None),
        P(),
    )
    return jax.shard_map(
        body, mesh=mesh, in_specs=placed, out_specs=P("exp", "tok", None), check_vma=False
    )
```
